128 devices in a mesh: fsdp: 16 (over x, z_lo, core), tensor: 8 (over y, z_hi).
Axes of the slice: x: 4, y: 4, z: 4 (z_hi: 2, z_lo: 2; z = z_hi * 2 + z_lo), core: 2. Of those that a mesh axis runs over, the one named last changes fastest.
Arguments:
- tokens: bfloat16 [16384, 4096], P('fsdp'), may hold values from -6 to 6
- input_source: float32 [256, 16, 4096], P('tensor', None, 'fsdp'), may hold values from -0.09375 to 0.09375
- branch_source: float32 [256, 16, 4096], P('tensor', None, 'fsdp'), may hold values from -0.09375 to 0.09375
- output_source: float32 [256, 16, 4096], P('tensor', None, 'fsdp'), may hold values from -0.09375 to 0.09375
- gates_source: float32 [2, 16, 256, 256], P(None, None, 'fsdp', 'tensor'), may hold values from -0.375 to 0.375
- decay_param: float32 [16, 256], replicated, may hold values from -9 to 1
- block_order: int32 [16], replicated, may hold values from 0 to 15, each once
Outputs:
- mixed: bfloat16 [16384, 4096], P('fsdp', 'tensor')
- input_serve: bfloat16 [4096, 4096], P(None, 'tensor')
- branch_serve: bfloat16 [4096, 4096], P(None, 'tensor')
- output_serve: bfloat16 [4096, 4096], P(None, 'tensor')
- gates_serve: bfloat16 [2, 16, 256, 256], P(None, 'tensor')
The draws below stay inside these ranges and needn't reach their ends.
Inputs may be any that keep to these rules, and one draw needn't show every extreme that they name: `block_order`: every gate block appears exactly once.
All inputs are finite; a program needn't handle non-finite values.
Results may differ from the reference program's by a relative error of at most 0.013.
Values may be sent and summed in bfloat16 or wider, within the bound.
No kernel may reach another device: no remote copies, remote signals or barrier semaphores. Data moves between devices by JAX's collectives and lax.ppermute only.
A program may use at most 128 MiB of HBM per device.

```python
import jax
import jax.numpy as jnp
from jax import lax

D = 4096
BLOCKS = 16
CHAN = 256
W = 4096
LEN = 256
TOK_DEV = 1024
TOKENS = 16384
N_TENSOR = 8


def shard_levels(rng, shape, cuts, least, largest):
    gain, own = 1.0, jax.random.fold_in(rng, 6)
    for dim, parts in cuts:
        steps = jnp.exp(jax.random.uniform(jax.random.fold_in(own, dim), (parts,), jnp.float32, least / len(cuts), largest / len(cuts)))
        gain = gain * jnp.repeat(steps, shape[dim] // parts).reshape([-1 if axis == dim else 1 for axis in range(len(shape))])
    return gain


def bell_draw(own_key, shape, scale, bound, cuts=(), held_as=jnp.bfloat16):
    level = shard_levels(own_key, shape, cuts, -0.22, 0.18) if cuts else 1.0
    entries = jax.random.normal(own_key, shape, jnp.float32) * scale * level
    return jnp.minimum(jnp.maximum(entries, -bound), bound).astype(held_as)


def setup_inputs(seed: int = 0) -> dict:
    key_of = jax.random.split(jax.random.key(seed), 8)
    tokens = bell_draw(key_of[0], (TOKENS, D), 1.0, 6.0, ((0, 16),))
    input_source = bell_draw(key_of[1], (CHAN, BLOCKS, D), D ** -0.5, 0.09375, ((0, 8), (2, 16)), jnp.float32)
    branch_source = bell_draw(key_of[2], (CHAN, BLOCKS, D), D ** -0.5, 0.09375, ((0, 8), (2, 16)), jnp.float32)
    output_source = bell_draw(key_of[3], (CHAN, BLOCKS, D), W ** -0.5, 0.09375, ((0, 8), (2, 16)), jnp.float32)
    gates_source = bell_draw(key_of[4], (2, BLOCKS, CHAN, CHAN), CHAN ** -0.5, 0.375, ((2, 16), (3, 8)), jnp.float32)
    decay_param = jnp.clip(jax.random.uniform(key_of[5], (BLOCKS, CHAN), jnp.float32, -9.0, 1.0), -9.0, 1.0)
    block_order = jax.random.permutation(key_of[6], BLOCKS).astype(jnp.int32)
    return {"tokens": tokens, "input_source": input_source, "branch_source": branch_source, "output_source": output_source, "gates_source": gates_source, "decay_param": decay_param, "block_order": block_order}


def serving_matrix(source, block_order):
    picked = jnp.take(source, block_order, axis=1)
    return jnp.transpose(picked, (2, 1, 0)).reshape(D, BLOCKS * CHAN).astype(jnp.bfloat16)

def combine_steps(earlier, latter):
    return (earlier[0] * latter[0], latter[0] * earlier[1] + latter[1])

def recurrence(features, input_serve, branch_serve, gates_serve, decay_rows):
    row_count = features.shape[0]
    branch_in = jnp.dot(features, input_serve, preferred_element_type=jnp.float32).astype(jnp.bfloat16)
    gate_pre = jnp.dot(features, branch_serve, preferred_element_type=jnp.float32)
    branch_wide = branch_in.astype(jnp.float32)
    blocked = branch_wide.reshape(row_count, BLOCKS, CHAN)
    gate_table = gates_serve.astype(jnp.float32)
    recur_pre = jnp.einsum('tbi,boi->tbo', blocked, gate_table[0]).reshape(row_count, -1)
    input_pre = jnp.einsum('tbi,boi->tbo', blocked, gate_table[1]).reshape(row_count, -1)
    recur_gate = jax.nn.sigmoid(recur_pre)
    input_gate = jax.nn.sigmoid(input_pre)
    log_decay = -8.0 * jax.nn.softplus(decay_rows) * recur_gate
    decay_step = jnp.exp(log_decay)
    drive_term = jnp.sqrt(1.0 - jnp.exp(2.0 * log_decay)) * (input_gate * branch_wide)
    replicas = row_count // TOK_DEV
    prompts = TOK_DEV // LEN
    shaped = (decay_step.reshape(replicas, LEN, prompts, -1), drive_term.reshape(replicas, LEN, prompts, -1))
    _, states = lax.associative_scan(combine_steps, shaped, axis=1)
    states = states.reshape(row_count, -1)
    return (states * jax.nn.gelu(gate_pre, approximate=True)).astype(jnp.bfloat16)

def reference(tokens, input_source, branch_source, output_source, gates_source, decay_param, block_order):
    input_serve = serving_matrix(input_source, block_order)
    branch_serve = serving_matrix(branch_source, block_order)
    output_serve = serving_matrix(output_source, block_order)
    gates_serve = jnp.transpose(jnp.take(gates_source, block_order, axis=1), (0, 1, 3, 2)).astype(jnp.bfloat16)
    decay_rows = jnp.take(decay_param, block_order, axis=0).reshape(BLOCKS * CHAN)
    gated = recurrence(tokens, input_serve, branch_serve, gates_serve, decay_rows)
    col_width = BLOCKS * CHAN // N_TENSOR
    running = jnp.zeros((tokens.shape[0], D), jnp.float32)
    for tp_group in range(N_TENSOR):
        lower = tp_group * col_width
        partial_value = jnp.dot(gated[:, lower:lower + col_width], output_serve[:, lower:lower + col_width].T, preferred_element_type=jnp.float32)
        rounded = lax.optimization_barrier(partial_value.astype(jnp.bfloat16))
        running = running + rounded.astype(jnp.float32)
    return (running.astype(jnp.bfloat16), input_serve, branch_serve, output_serve, gates_serve)
```

```python
import jax
import jax.numpy as jnp
from jax import lax
from jax.experimental import pallas as pl
from jax.experimental.pallas import tpu as pltpu
from jax.sharding import PartitionSpec as P


LEN = 256
BF = jnp.bfloat16
F32 = jnp.float32


def fsdp_perm(dx=0, dz=0, dc=0):
    out = []
    for f in range(16):
        x, z, c = f // 4, (f // 2) % 2, f % 2
        out.append((f, (((x + dx) % 4) * 2 + (z ^ dz)) * 2 + (c ^ dc)))
    return out


def tensor_perm(dy=0, dz=0):
    return [(t, ((t // 2 + dy) % 4) * 2 + ((t % 2) ^ dz)) for t in range(8)]


def send_x(a, dx):
    return lax.ppermute(a, "fsdp", fsdp_perm(dx=dx))


def send_z(a):
    return lax.ppermute(a, "fsdp", fsdp_perm(dz=1))


def send_core(a):
    return lax.ppermute(a, "fsdp", fsdp_perm(dc=1))


def send_y(a, dy):
    return lax.ppermute(a, "tensor", tensor_perm(dy=dy))


def send_zhi(a):
    return lax.ppermute(a, "tensor", tensor_perm(dz=1))


SLOT_X_ZFIRST = (0, 0, -1, -1, 1, 1, 2, 2)
SLOT_Z_ZFIRST = (0, 1, 0, 1, 0, 1, 0, 1)
SLOT_X_XFIRST = (0, -1, 1, 2, 0, -1, 1, 2)
SLOT_Z_XFIRST = (0, 0, 0, 0, 1, 1, 1, 1)


def gather_z_first(q):
    other = send_z(q)
    pair = jnp.stack([q, other])
    left = send_x(pair, 1)
    right = send_x(pair, -1)
    far_own = send_x(left[0], 1)
    far_other = send_x(right[1], -1)
    own = jnp.concatenate([pair, left, right, far_own[None], far_other[None]])
    return own, send_core(own)


def gather_x_first(q):
    half = q.shape[0] // 2
    left = send_x(q, 1)
    right = send_x(q, -1)
    far_top = send_x(left[:half], 1)
    far_low = send_x(right[half:], -1)
    row = jnp.stack([q, left, right, jnp.concatenate([far_top, far_low])])
    other = send_z(row)
    own = jnp.concatenate([row, other])
    return own, send_core(own)


def place_kernel(extra, meta, own_ref, peer_ref, *outs):
    core = meta[16]
    outs[0][0, 0, core] = own_ref[0, :256]
    outs[0][0, 0, 1 - core] = peer_ref[0, :256]
    if extra:
        outs[1][0, 0, core] = own_ref[0, 256:]
        outs[1][0, 0, 1 - core] = peer_ref[0, 256:]


def place(own, peer, slot_x, slot_z):
    f = lax.axis_index("fsdp")
    x, z, core = f // 4, (f // 2) % 2, f % 2
    meta = jnp.concatenate(
        [
            (x + jnp.array(slot_x, jnp.int32) + 4) % 4,
            (z + jnp.array(slot_z, jnp.int32)) % 2,
            core[None],
        ]
    ).astype(jnp.int32)
    rows = own.shape[1]
    extra = rows - 256
    shapes = [jax.ShapeDtypeStruct((4, 2, 2, 256, 512), BF)]
    out_specs = [pl.BlockSpec((1, 1, 2, 256, 512), lambda s, m: (m[s], m[8 + s], 0, 0, 0))]
    if extra:
        shapes.append(jax.ShapeDtypeStruct((4, 2, 2, extra, 512), BF))
        out_specs.append(pl.BlockSpec((1, 1, 2, extra, 512), lambda s, m: (m[s], m[8 + s], 0, 0, 0)))
    spec = pl.BlockSpec((1, rows, 512), lambda s, m: (s, 0, 0))
    res = pl.pallas_call(
        lambda *refs: place_kernel(extra, *refs),
        out_shape=shapes,
        grid_spec=pltpu.PrefetchScalarGridSpec(
            num_scalar_prefetch=1, grid=(8,), in_specs=[spec, spec], out_specs=out_specs
        ),
        cost_estimate=pl.CostEstimate(flops=4_000_000, bytes_accessed=8 << 20, transcendentals=0),
        name="place",
    )(meta, own, peer)
    return (res[0].reshape(4096, 512), res[1].reshape(16, extra, 512)) if extra else res[0].reshape(4096, 512)


CH = 128


def scan_kernel(bi_ref, g_ref, rate_ref, out_ref):
    rate = rate_ref[...]
    low = lax.broadcasted_iota(jnp.int32, (CH // 8, 8, 256), 1) < 4
    dims = (((1,), (1,)), ((), ()))

    def chunk(n, carry):
        rows = pl.ds(pl.multiple_of(n * CH, CH), CH)
        bi = bi_ref[rows, :]
        pre_r = lax.dot_general(bi, g_ref[0, 0], dims, preferred_element_type=F32)
        pre_i = lax.dot_general(bi, g_ref[1, 0], dims, preferred_element_type=F32)
        log_a = -8.0 * rate * jax.nn.sigmoid(pre_r)
        a = jnp.exp(log_a)
        d = jnp.sqrt(1.0 - jnp.exp(2.0 * log_a)) * (jax.nn.sigmoid(pre_i) * bi.astype(F32))
        a = a.reshape(CH // 8, 8, 256)
        d = d.reshape(CH // 8, 8, 256)
        a_prev = jnp.where(low, 1.0, pltpu.roll(a, 4, 1))
        d_prev = jnp.where(low, 0.0, pltpu.roll(d, 4, 1))
        d = a * d_prev + d
        a = a * a_prev
        a_end = jnp.where(low, pltpu.roll(a, 4, 1), a)
        d_end = jnp.where(low, pltpu.roll(d, 4, 1), d)
        states = []
        for k in range(CH // 8):
            states.append(a[k] * carry + d[k])
            carry = a_end[k] * carry + d_end[k]
        out_ref[rows, :] = jnp.concatenate(states, axis=0)
        return carry

    lax.fori_loop(0, 1024 // CH, chunk, jnp.zeros((8, 256), F32))


def gate_scan(branch_in, gates, rate):
    return pl.pallas_call(
        scan_kernel,
        out_shape=jax.ShapeDtypeStruct((1024, 512), F32),
        grid=(2,),
        in_specs=[
            pl.BlockSpec((1024, 256), lambda j: (0, j)),
            pl.BlockSpec((2, 1, 256, 256), lambda j: (0, j, 0, 0)),
            pl.BlockSpec((1, 256), lambda j: (0, j)),
        ],
        out_specs=pl.BlockSpec((1024, 256), lambda j: (0, j)),
        cost_estimate=pl.CostEstimate(
            flops=8_000_000_000, bytes_accessed=4 << 20, transcendentals=4 << 20
        ),
        name="gate_scan",
    )(branch_in, gates, rate)


RY = 576
HY = RY // 2
RZ = 1024 - RY
HZ = RZ // 2


def plus(*terms):
    total = terms[0].astype(F32)
    for term in terms[1:]:
        total = total + term.astype(F32)
    return total.astype(BF)


def project_and_scatter(gated, output_serve):
    t = lax.axis_index("tensor")
    y, zh = t // 2, t % 2
    dims = (((1,), (1,)), ((), ()))

    def part(rows, start, width):
        w = lax.dynamic_slice_in_dim(output_serve, start, width)
        return lax.dot_general(rows, w, dims, preferred_element_type=F32).astype(BF)

    gy, gz = gated[:RY], gated[RY:]
    starts = {r: ((y + r) % 4) * 1024 for r in (2, 1, 3, 0)}

    sent, kept = {}, {}
    for r in (2, 1, 3, 0):
        sent[r] = part(gz, starts[r] + (1 - zh) * 512, 512)
        kept[r] = part(gz, starts[r] + zh * 512, 512)
    back_far = send_zhi(sent[2])
    far = part(gy, starts[2], 1024)
    from_left = send_y(far[:HY], 1)
    from_right = send_y(far[HY:], -1)
    back_rest = send_zhi(jnp.stack([sent[1], sent[3], sent[0]]))
    up = part(gy, starts[1], 1024)
    down = part(gy, starts[3], 1024)
    mine = part(gy, starts[0], 1024)
    up = jnp.concatenate([plus(up[:HY], from_left), up[HY:]])
    down = jnp.concatenate([down[:HY], plus(down[HY:], from_right)])
    in_left = send_y(up, 1)
    in_right = send_y(down, -1)

    zfar = plus(kept[2], back_far)
    zfrom_left = send_y(zfar[:HZ], 1)
    zfrom_right = send_y(zfar[HZ:], -1)

    total = plus(mine, in_left, in_right)
    give = lax.dynamic_slice_in_dim(total, (1 - zh) * 512, 512, axis=1)
    keep = lax.dynamic_slice_in_dim(total, zh * 512, 512, axis=1)
    out_y = plus(keep, send_zhi(give))

    zup = jnp.concatenate(
        [plus(kept[1][:HZ], back_rest[0, :HZ], zfrom_left), plus(kept[1][HZ:], back_rest[0, HZ:])]
    )
    zdown = jnp.concatenate(
        [plus(kept[3][:HZ], back_rest[1, :HZ]), plus(kept[3][HZ:], back_rest[1, HZ:], zfrom_right)]
    )
    zin_left = send_y(zup, 1)
    zin_right = send_y(zdown, -1)
    out_z = plus(kept[0], back_rest[2], zin_left, zin_right)
    return jnp.concatenate([out_y, out_z])


def on_device(
    tokens, input_source, branch_source, output_source, gates_source, decay_param, block_order
):
    t = lax.axis_index("tensor")
    own_blocks = lax.dynamic_slice_in_dim(block_order, t * 2, 2)

    def section(w):
        picked = jnp.take(w.astype(BF), block_order, axis=1)
        return jnp.transpose(picked, (1, 0, 2)).reshape(8, 64, 256)

    gates_picked = jnp.take(gates_source.astype(BF), block_order, axis=1)
    gates_flat = jnp.transpose(gates_picked.reshape(2, 8, 2, 16, 32), (1, 0, 2, 3, 4)).reshape(8, 8, 256)
    packed = jnp.concatenate(
        [section(input_source), section(branch_source), section(output_source), gates_flat], axis=1
    )
    swapped = lax.all_to_all(packed, "tensor", 0, 0, tiled=True)

    def piece(n):
        part = swapped[:, n * 64 : (n + 1) * 64].reshape(8, 2, 32, 256)
        return jnp.transpose(part, (3, 1, 0, 2)).reshape(256, 512)

    gate_part = swapped[:, 192:200].reshape(8, 2, 2, 16, 32)
    gate_rows = jnp.transpose(gate_part, (1, 2, 3, 0, 4)).reshape(32, 512)

    in_own, in_peer = gather_z_first(jnp.concatenate([piece(0), gate_rows]))
    input_serve, gate_all = place(in_own, in_peer, SLOT_X_ZFIRST, SLOT_Z_ZFIRST)
    br_own, br_peer = gather_x_first(piece(1))
    branch_serve = place(br_own, br_peer, SLOT_X_XFIRST, SLOT_Z_XFIRST)
    out_own, out_peer = gather_z_first(piece(2))
    output_serve = place(out_own, out_peer, SLOT_X_ZFIRST, SLOT_Z_ZFIRST)

    gates_serve = jnp.transpose(gate_all.reshape(16, 2, 2, 16, 256), (1, 2, 4, 0, 3)).reshape(2, 2, 256, 256)
    rate = jax.nn.softplus(jnp.take(decay_param, own_blocks, axis=0)).reshape(1, 512)
    branch_in = jnp.dot(tokens, input_serve, preferred_element_type=F32).astype(BF)
    states = gate_scan(branch_in, gates_serve, rate)
    gate_pre = jnp.dot(tokens, branch_serve, preferred_element_type=F32)
    gated = (states * jax.nn.gelu(gate_pre, approximate=True)).astype(BF)
    mixed = project_and_scatter(gated, output_serve)
    return (mixed, input_serve, branch_serve, output_serve, gates_serve)


def solution(mesh):
    return jax.shard_map(
        on_device,
        mesh=mesh,
        in_specs=(
            P("fsdp", None),
            P("tensor", None, "fsdp"),
            P("tensor", None, "fsdp"),
            P("tensor", None, "fsdp"),
            P(None, None, "fsdp", "tensor"),
            P(),
            P(),
        ),
        out_specs=(
            P("fsdp", "tensor"),
            P(None, "tensor"),
            P(None, "tensor"),
            P(None, "tensor"),
            P(None, "tensor", None, None),
        ),
        check_vma=False,
    )
```

```python
import jax
import jax.numpy as jnp
from jax import lax
from jax.experimental import pallas as pl
from jax.experimental.pallas import tpu as pltpu
from jax.sharding import PartitionSpec as P


BF = jnp.bfloat16
F32 = jnp.float32


def fsdp_perm(dx=0, dz=0, dc=0):
    out = []
    for f in range(16):
        x, z, c = f // 4, (f // 2) % 2, f % 2
        out.append((f, (((x + dx) % 4) * 2 + (z ^ dz)) * 2 + (c ^ dc)))
    return out


def tensor_perm(dy=0, dz=0):
    return [(t, ((t // 2 + dy) % 4) * 2 + ((t % 2) ^ dz)) for t in range(8)]


CH = 128


def scan_kernel(bi_ref, g_ref, rate_ref, out_ref):
    rate = rate_ref[...]
    low = lax.broadcasted_iota(jnp.int32, (CH // 8, 8, 256), 1) < 4
    dims = (((1,), (1,)), ((), ()))

    def chunk(n, carry):
        rows = pl.ds(pl.multiple_of(n * CH, CH), CH)
        bi = bi_ref[rows, :]
        pre_r = lax.dot_general(bi, g_ref[0, 0], dims, preferred_element_type=F32)
        pre_i = lax.dot_general(bi, g_ref[1, 0], dims, preferred_element_type=F32)
        log_a = -8.0 * rate * jax.nn.sigmoid(pre_r)
        a = jnp.exp(log_a)
        d = jnp.sqrt(1.0 - jnp.exp(2.0 * log_a)) * (jax.nn.sigmoid(pre_i) * bi.astype(F32))
        a = a.reshape(CH // 8, 8, 256)
        d = d.reshape(CH // 8, 8, 256)
        a_prev = jnp.where(low, 1.0, pltpu.roll(a, 4, 1))
        d_prev = jnp.where(low, 0.0, pltpu.roll(d, 4, 1))
        d = a * d_prev + d
        a = a * a_prev
        a_end = jnp.where(low, pltpu.roll(a, 4, 1), a)
        d_end = jnp.where(low, pltpu.roll(d, 4, 1), d)
        states = []
        for k in range(CH // 8):
            states.append(a[k] * carry + d[k])
            carry = a_end[k] * carry + d_end[k]
        out_ref[rows, :] = jnp.concatenate(states, axis=0)
        return carry

    lax.fori_loop(0, 1024 // CH, chunk, jnp.zeros((8, 256), F32))


def gate_scan(branch_in, gates, rate):
    return pl.pallas_call(
        scan_kernel,
        out_shape=jax.ShapeDtypeStruct((1024, 512), F32),
        grid=(2,),
        in_specs=[
            pl.BlockSpec((1024, 256), lambda j: (0, j)),
            pl.BlockSpec((2, 1, 256, 256), lambda j: (0, j, 0, 0)),
            pl.BlockSpec((1, 256), lambda j: (0, j)),
        ],
        out_specs=pl.BlockSpec((1024, 256), lambda j: (0, j)),
        cost_estimate=pl.CostEstimate(
            flops=8_000_000_000, bytes_accessed=4 << 20, transcendentals=4 << 20
        ),
        name="gate_scan",
    )(branch_in, gates, rate)


def send_x(a, dx):
    return lax.ppermute(a, "fsdp", fsdp_perm(dx=dx))


def send_z(a):
    return lax.ppermute(a, "fsdp", fsdp_perm(dz=1))


def send_core(a):
    return lax.ppermute(a, "fsdp", fsdp_perm(dc=1))


def send_y(a, dy):
    return lax.ppermute(a, "tensor", tensor_perm(dy=dy))


def send_zhi(a):
    return lax.ppermute(a, "tensor", tensor_perm(dz=1))


CHUNKS = (640, 384)


def position():
    f = lax.axis_index("fsdp")
    t = lax.axis_index("tensor")
    return f // 4, (f // 2) % 2, f % 2, t // 2, t % 2


def slot_meta(dx):
    x, z, core, _, _ = position()
    at = (x + jnp.array(dx, jnp.int32) + 4) & 3
    return jnp.concatenate([at, core[None], z[None]]).astype(jnp.int32)


def put(w_ref, core, z, owns, peers):
    for j in range(2):
        at = jnp.bitwise_xor(z, j)
        w_ref[at, core] = owns[j]
        w_ref[at, 1 - core] = peers[j]


def place_kernel(meta, own_ref, peer_ref, w_ref):
    core, z = meta[4], meta[5]
    put(w_ref, core, z, (own_ref[0, 0], own_ref[1, 0]), (peer_ref[0, 0], peer_ref[1, 0]))


def place(meta, own, peer):
    src = pl.BlockSpec((2, 1, 256, 512), lambda s, m: (0, s, 0, 0))
    w = pl.pallas_call(
        place_kernel,
        out_shape=jax.ShapeDtypeStruct((8, 2, 256, 512), BF),
        grid_spec=pltpu.PrefetchScalarGridSpec(
            num_scalar_prefetch=1,
            grid=(4,),
            in_specs=[src, src],
            out_specs=pl.BlockSpec((2, 2, 256, 512), lambda s, m: (m[s], 0, 0, 0)),
        ),
        cost_estimate=pl.CostEstimate(flops=4_000_000, bytes_accessed=8 << 20, transcendentals=0),
        name="place",
    )(meta, own, peer)
    return w.reshape(4096, 512)


def matmul_kernel(steps, extra, tail, meta, *refs):
    refs = list(refs)
    tok_ref, own_ref, peer_ref = refs[:3]
    refs = refs[3:]
    core, z = meta[steps], meta[steps + 1]
    step = pl.program_id(0)
    if tail:
        before_ref = refs.pop(0)
        refs.pop(0)
        if extra:
            refs.pop(0)
        else:
            state_ref = refs.pop(0)
    w_ref = refs.pop(0)
    put(w_ref, core, z, (own_ref[0, :256], own_ref[1, :256]), (peer_ref[0, :256], peer_ref[1, :256]))
    if extra:
        g_ref = refs.pop(0)
        put(g_ref, core, z, (own_ref[0, 256:], own_ref[1, 256:]), (peer_ref[0, 256:], peer_ref[1, 256:]))
    w = w_ref[...].reshape(1024, 512)
    if not tail:
        acc_ref = refs.pop(0)

        @pl.when(step == 0)
        def _():
            acc_ref[...] = jnp.dot(tok_ref[...], w, preferred_element_type=F32)

        @pl.when(step > 0)
        def _():
            acc_ref[...] += jnp.dot(tok_ref[...], w, preferred_element_type=F32)

    elif extra:
        out_ref = refs.pop(0)
        out_ref[...] = (before_ref[...] + jnp.dot(tok_ref[...], w, preferred_element_type=F32)).astype(BF)
    else:
        acc_ref = refs.pop()
        acc_ref[...] = before_ref[...] + jnp.dot(tok_ref[...], w, preferred_element_type=F32)
        base = 0
        for size, out_ref in zip(CHUNKS, refs):

            def rows_step(n, _, base=base, out_ref=out_ref):
                rows = pl.ds(pl.multiple_of(base + n * 32, 32), 32)
                value = state_ref[rows, :] * jax.nn.gelu(acc_ref[rows, :], approximate=True)
                out_ref[pl.ds(pl.multiple_of(n * 32, 32), 32), :] = value.astype(BF)
                return 0

            lax.fori_loop(0, size // 32, rows_step, 0)
            base += size


def whole(shape):
    return pl.BlockSpec(shape, lambda s, m: (0,) * len(shape))


def matmul_part(meta, tokens, own, peer, extra, before=None, w=None, g=None, states=None):
    rows = 256 + extra
    steps = own.shape[0] // 2
    tail = before is not None
    src = pl.BlockSpec((2, rows, 512), lambda s, m: (s, 0, 0))
    operands = [tokens, own, peer]
    in_specs = [pl.BlockSpec((1024, 1024), lambda s, m: (0, m[s])), src, src]
    aliases = {}
    scratch = []
    out_shape = [jax.ShapeDtypeStruct((8, 2, 256, 512), BF)]
    out_specs = [pl.BlockSpec((2, 2, 256, 512), lambda s, m: (m[s], 0, 0, 0))]
    if extra:
        out_shape.append(jax.ShapeDtypeStruct((8, 2, extra, 512), BF))
        out_specs.append(pl.BlockSpec((2, 2, extra, 512), lambda s, m: (m[s], 0, 0, 0)))
    if tail:
        operands += [before, w]
        in_specs += [whole((1024, 512)), pl.BlockSpec(memory_space=pl.ANY)]
        aliases = {5: 0}
        if extra:
            operands.append(g)
            in_specs.append(pl.BlockSpec(memory_space=pl.ANY))
            aliases[6] = 1
            out_shape.append(jax.ShapeDtypeStruct((1024, 512), BF))
            out_specs.append(whole((1024, 512)))
        else:
            operands.append(states)
            in_specs.append(whole((1024, 512)))
            out_shape += [jax.ShapeDtypeStruct((size, 512), BF) for size in CHUNKS]
            out_specs += [whole((size, 512)) for size in CHUNKS]
            scratch = [pltpu.VMEM((1024, 512), F32)]
    else:
        out_shape.append(jax.ShapeDtypeStruct((1024, 512), F32))
        out_specs.append(whole((1024, 512)))
    return pl.pallas_call(
        lambda *refs: matmul_kernel(steps, extra, tail, *refs),
        out_shape=out_shape,
        grid_spec=pltpu.PrefetchScalarGridSpec(
            num_scalar_prefetch=1,
            grid=(steps,),
            in_specs=in_specs,
            out_specs=out_specs,
            scratch_shapes=scratch,
        ),
        input_output_aliases=aliases,
        cost_estimate=pl.CostEstimate(
            flops=1_000_000_000 * steps, bytes_accessed=(4 << 20) * steps, transcendentals=0
        ),
    )(meta, *operands)


def project_kernel(meta, g0, g1, g3, fa, fb, own_ref, peer_ref, give_ref, keep_ref, far_ref):
    core = meta[1]
    half = fa.shape[0]
    dims = (((1,), (1,)), ((), ()))
    step = pl.program_id(0)

    @pl.when(step == 0)
    def _():
        far_ref[:half] = fa[...]
        far_ref[half:] = fb[...]

    def side(out_ref):
        for w_ref, at in ((own_ref, core), (peer_ref, 1 - core)):
            cols = pl.ds(pl.multiple_of(at * 256, 256), 256)
            acc = lax.dot_general(g0[...], w_ref[0, 0], dims, preferred_element_type=F32)
            acc += lax.dot_general(g1[...], w_ref[1, 0], dims, preferred_element_type=F32)
            acc += lax.dot_general(far_ref[...], w_ref[2, 0], dims, preferred_element_type=F32)
            acc += lax.dot_general(g3[...], w_ref[3, 0], dims, preferred_element_type=F32)
            out_ref[:, cols] = acc.astype(out_ref.dtype)

    @pl.when(step == 0)
    def _():
        side(give_ref)

    @pl.when(step == 1)
    def _():
        side(keep_ref)


def project(meta, gs, w_own, w_peer):
    size = gs[0].shape[0]
    wspec = pl.BlockSpec((4, 1, 256, 512), lambda s, m: (0, jnp.bitwise_xor(m[0], s), 0, 0))
    return pl.pallas_call(
        project_kernel,
        out_shape=[
            jax.ShapeDtypeStruct((size, 512), BF),
            jax.ShapeDtypeStruct((size, 512), F32),
        ],
        grid_spec=pltpu.PrefetchScalarGridSpec(
            num_scalar_prefetch=1,
            grid=(2,),
            in_specs=[whole(g.shape) for g in gs] + [wspec, wspec],
            out_specs=[whole((size, 512))] * 2,
            scratch_shapes=[pltpu.VMEM((size, 512), BF)],
        ),
        cost_estimate=pl.CostEstimate(
            flops=size * 2048 * 2048, bytes_accessed=8 << 20, transcendentals=0
        ),
        name="project",
    )(meta, *gs, w_own, w_peer)


def gather_z_first(q):
    other = send_z(q)
    pair = jnp.stack([q, other])
    left = send_x(pair, 1)
    right = send_x(pair, -1)
    far_own = send_x(left[0], 1)
    far_other = send_x(right[1], -1)
    near = jnp.concatenate([pair, left, right])
    far = jnp.stack([far_own, far_other])
    return near, send_core(near), far, send_core(far)


def on_device(
    tokens, input_source, branch_source, output_source, gates_source, decay_param, block_order
):
    x, z, core, y, zh = position()
    own_blocks = lax.dynamic_slice_in_dim(block_order, (y * 2 + zh) * 2, 2)

    def section(w):
        picked = jnp.take(w.astype(BF), block_order, axis=1)
        return jnp.transpose(picked, (1, 0, 2)).reshape(8, 64, 256)

    gates_picked = jnp.take(gates_source.astype(BF), block_order, axis=1)
    gates_flat = jnp.transpose(gates_picked.reshape(2, 8, 2, 16, 32), (1, 0, 2, 3, 4)).reshape(8, 8, 256)
    packed = jnp.concatenate(
        [section(input_source), section(branch_source), section(output_source), gates_flat], axis=1
    )
    swapped = lax.all_to_all(packed, "tensor", 0, 0, tiled=True)

    def piece(n):
        part = swapped[:, n * 64 : (n + 1) * 64].reshape(8, 2, 32, 256)
        return jnp.transpose(part, (3, 1, 0, 2)).reshape(256, 512)

    gate_part = swapped[:, 192:200].reshape(8, 2, 2, 16, 32)
    gate_rows = jnp.transpose(gate_part, (1, 2, 3, 0, 4)).reshape(32, 512)

    near_meta = slot_meta((0, -1, 1))
    far_meta = slot_meta((2,))
    row_meta = slot_meta((0, 1, 2, 3))

    q = piece(2)
    left = send_x(q, 1)
    right = send_x(q, -1)
    far_top = send_x(left[:128], 1)
    far_low = send_x(right[128:], -1)
    row = jnp.stack([q, right, jnp.concatenate([far_top, far_low]), left])
    other_row = send_z(row)

    def along_y(row):
        got = [lax.dynamic_index_in_dim(row, (y - x) & 3, 0, keepdims=False)]
        for r in (1, 2, 3):
            block = lax.dynamic_index_in_dim(row, (y - r - x) & 3, 0, keepdims=False)
            got.append(send_y(block, -r))
        return jnp.stack(got)

    w_own = jnp.stack([along_y(row), along_y(other_row)], axis=1)
    w_peer = send_core(w_own)
    out_own = jnp.stack([row, other_row])
    out_peer = send_core(out_own)

    in_near, in_near_peer, in_far, in_far_peer = gather_z_first(
        jnp.concatenate([piece(0), gate_rows])
    )
    br_near, br_near_peer, br_far, br_far_peer = gather_z_first(piece(1))

    w, g, acc = matmul_part(near_meta, tokens, in_near, in_near_peer, 32)
    w, g, branch_in = matmul_part(far_meta, tokens, in_far, in_far_peer, 32, before=acc, w=w, g=g)
    input_serve = w.reshape(4096, 512)
    gate_all = g.reshape(16, 32, 512)
    gates_serve = jnp.transpose(gate_all.reshape(16, 2, 2, 16, 256), (1, 2, 4, 0, 3)).reshape(2, 2, 256, 256)
    rate = jax.nn.softplus(jnp.take(decay_param, own_blocks, axis=0)).reshape(1, 512)
    states = gate_scan(branch_in, gates_serve, rate)
    w, acc = matmul_part(near_meta, tokens, br_near, br_near_peer, 0)
    w, *gated = matmul_part(
        far_meta, tokens, br_far, br_far_peer, 0, before=acc, w=w, states=states
    )
    branch_serve = w.reshape(4096, 512)
    output_serve = place(row_meta, out_own, out_peer)

    give_meta = jnp.stack([(1 - zh) ^ z, core]).astype(jnp.int32)
    parts = []
    for g in gated:
        half = g.shape[0] // 2
        below = send_y(g, 1)
        above = send_y(g, -1)
        far_a = send_y(below[:half], 1)
        far_b = send_y(above[half:], -1)
        terms = (g, above, below, far_a, far_b)
        give, keep = project(give_meta, terms, w_own, w_peer)
        got = send_zhi(give)
        parts.append((keep + got.astype(F32)).astype(BF))
    mixed = jnp.concatenate(parts)
    return (mixed, input_serve, branch_serve, output_serve, gates_serve)


def solution(mesh):
    return jax.shard_map(
        on_device,
        mesh=mesh,
        in_specs=(
            P("fsdp", None),
            P("tensor", None, "fsdp"),
            P("tensor", None, "fsdp"),
            P("tensor", None, "fsdp"),
            P(None, None, "fsdp", "tensor"),
            P(),
            P(),
        ),
        out_specs=(
            P("fsdp", "tensor"),
            P(None, "tensor"),
            P(None, "tensor"),
            P(None, "tensor"),
            P(None, "tensor", None, None),
        ),
        check_vma=False,
    )
```

```python
import jax
import jax.numpy as jnp
from jax import lax
from jax.experimental import pallas as pl
from jax.experimental.pallas import tpu as pltpu
from jax.sharding import PartitionSpec as P


BF = jnp.bfloat16
F32 = jnp.float32


def fsdp_perm(dx=0, dz=0, dc=0):
    out = []
    for f in range(16):
        x, z, c = f // 4, (f // 2) % 2, f % 2
        out.append((f, (((x + dx) % 4) * 2 + (z ^ dz)) * 2 + (c ^ dc)))
    return out


def tensor_perm(dy=0, dz=0):
    return [(t, ((t // 2 + dy) % 4) * 2 + ((t % 2) ^ dz)) for t in range(8)]


CH = 128
BIG = pltpu.CompilerParams(vmem_limit_bytes=60 << 20)


def scan_kernel(bi_ref, g_ref, rate_ref, out_ref, gates_ref):
    rate = rate_ref[...]
    low = lax.broadcasted_iota(jnp.int32, (CH // 8, 8, 256), 1) < 4
    w_r = g_ref[:, :16].reshape(256, 256)
    w_i = g_ref[:, 16:].reshape(256, 256)
    gates_ref[0, 0] = w_r.T
    gates_ref[1, 0] = w_i.T

    def chunk(n, carry):
        rows = pl.ds(pl.multiple_of(n * CH, CH), CH)
        bi = bi_ref[rows, :]
        pre_r = jnp.dot(bi, g_ref[:, :16].reshape(256, 256), preferred_element_type=F32)
        pre_i = jnp.dot(bi, g_ref[:, 16:].reshape(256, 256), preferred_element_type=F32)
        a = jnp.exp(rate * jax.nn.sigmoid(pre_r))
        d = jnp.sqrt(1.0 - a * a) * (jax.nn.sigmoid(pre_i) * bi.astype(F32))
        a = a.reshape(CH // 8, 8, 256)
        d = d.reshape(CH // 8, 8, 256)
        a_prev = jnp.where(low, 1.0, pltpu.roll(a, 4, 1))
        d_prev = jnp.where(low, 0.0, pltpu.roll(d, 4, 1))
        d = a * d_prev + d
        a = a * a_prev
        a_end = jnp.where(low, pltpu.roll(a, 4, 1), a)
        d_end = jnp.where(low, pltpu.roll(d, 4, 1), d)
        states = []
        for k in range(CH // 8):
            states.append(a[k] * carry + d[k])
            carry = a_end[k] * carry + d_end[k]
        out_ref[rows, :] = jnp.concatenate(states, axis=0)
        return carry

    lax.fori_loop(0, 1024 // CH, chunk, jnp.zeros((8, 256), F32))


def gate_scan(branch_in, gates, rate):
    return pl.pallas_call(
        scan_kernel,
        out_shape=[
            jax.ShapeDtypeStruct((1024, 512), F32),
            jax.ShapeDtypeStruct((2, 2, 256, 256), BF),
        ],
        grid=(2,),
        in_specs=[
            pl.BlockSpec((1024, 256), lambda j: (0, j)),
            pl.BlockSpec((16, 32, 256), lambda j: (0, 0, j)),
            pl.BlockSpec((1, 256), lambda j: (0, j)),
        ],
        out_specs=[
            pl.BlockSpec((1024, 256), lambda j: (0, j)),
            pl.BlockSpec((2, 1, 256, 256), lambda j: (0, j, 0, 0)),
        ],
        compiler_params=BIG,
        cost_estimate=pl.CostEstimate(
            flops=8_000_000_000, bytes_accessed=4 << 20, transcendentals=4 << 20
        ),
        name="gate_scan",
    )(branch_in, gates, rate)


def send_x(a, dx):
    return lax.ppermute(a, "fsdp", fsdp_perm(dx=dx))


def send_z(a):
    return lax.ppermute(a, "fsdp", fsdp_perm(dz=1))


def send_core(a):
    return lax.ppermute(a, "fsdp", fsdp_perm(dc=1))


def send_y(a, dy):
    return lax.ppermute(a, "tensor", tensor_perm(dy=dy))


def send_zhi(a):
    return lax.ppermute(a, "tensor", tensor_perm(dz=1))


CHUNKS = (448, 576)


def position():
    f = lax.axis_index("fsdp")
    t = lax.axis_index("tensor")
    return f // 4, (f // 2) % 2, f % 2, t // 2, t % 2


def slot_meta(dx):
    x, z, core, _, _ = position()
    at = (x + jnp.array(dx, jnp.int32) + 4) & 3
    return jnp.concatenate([at, core[None], z[None]]).astype(jnp.int32)


def put(w_ref, core, z, owns, peers):
    for j in range(2):
        at = jnp.bitwise_xor(z, j)
        w_ref[at, core] = owns[j]
        w_ref[at, 1 - core] = peers[j]


def place_kernel(meta, own0, own1, peer0, peer1, w_ref):
    core, z = meta[4], meta[5]
    put(w_ref, core, z, (own0[0], own1[0]), (peer0[0], peer1[0]))


def place(meta, owns, peers):
    src = pl.BlockSpec((1, 256, 512), lambda s, m: (s, 0, 0))
    w = pl.pallas_call(
        place_kernel,
        out_shape=jax.ShapeDtypeStruct((8, 2, 256, 512), BF),
        grid_spec=pltpu.PrefetchScalarGridSpec(
            num_scalar_prefetch=1,
            grid=(4,),
            in_specs=[src] * 4,
            out_specs=pl.BlockSpec((2, 2, 256, 512), lambda s, m: (m[s], 0, 0, 0)),
        ),
        compiler_params=BIG,
        cost_estimate=pl.CostEstimate(flops=4_000_000, bytes_accessed=8 << 20, transcendentals=0),
        name="place",
    )(meta, *owns, *peers)
    return w.reshape(4096, 512)


def matmul_kernel(extra, meta, tok_ref, near_ref, near_peer_ref, far_ref, far_peer_ref, *refs):
    if extra:
        w_ref, g_ref, out_ref, acc_ref = refs
    else:
        state_ref, w_ref, *out_refs, acc_ref = refs
    core, z = meta[4], meta[5]
    step = pl.program_id(0)

    def put_all(own_ref, peer_ref):
        put(w_ref, core, z, (own_ref[0, :256], own_ref[1, :256]), (peer_ref[0, :256], peer_ref[1, :256]))
        if extra:
            put(g_ref, core, z, (own_ref[0, 256:], own_ref[1, 256:]), (peer_ref[0, 256:], peer_ref[1, 256:]))

    @pl.when(step < 3)
    def _():
        put_all(near_ref, near_peer_ref)

    @pl.when(step == 3)
    def _():
        put_all(far_ref, far_peer_ref)

    w = w_ref[...].reshape(1024, 512)

    @pl.when(step == 0)
    def _():
        acc_ref[...] = jnp.dot(tok_ref[...], w, preferred_element_type=F32)

    @pl.when(step > 0)
    def _():
        acc_ref[...] += jnp.dot(tok_ref[...], w, preferred_element_type=F32)

    @pl.when(step == 3)
    def _():
        if extra:
            out_ref[...] = acc_ref[...].astype(BF)
        else:
            base = 0
            for size, part_ref in zip(CHUNKS, out_refs):

                def rows_step(n, _, base=base, part_ref=part_ref):
                    rows = pl.ds(pl.multiple_of(base + n * 32, 32), 32)
                    value = state_ref[rows, :] * jax.nn.gelu(acc_ref[rows, :], approximate=True)
                    part_ref[pl.ds(pl.multiple_of(n * 32, 32), 32), :] = value.astype(BF)
                    return 0

                lax.fori_loop(0, size // 32, rows_step, 0)
                base += size


def whole(shape):
    return pl.BlockSpec(shape, lambda s, m: (0,) * len(shape))


def matmul(meta, tokens, parts, extra, states=None):
    rows = 256 + extra
    near = pl.BlockSpec((2, rows, 512), lambda s, m: (jnp.minimum(s, 2), 0, 0))
    operands = [tokens, *parts]
    in_specs = [pl.BlockSpec((1024, 1024), lambda s, m: (0, m[s])), near, near]
    in_specs += [whole((2, rows, 512))] * 2
    out_shape = [jax.ShapeDtypeStruct((8, 2, 256, 512), BF)]
    out_specs = [pl.BlockSpec((2, 2, 256, 512), lambda s, m: (m[s], 0, 0, 0))]
    if extra:
        out_shape += [jax.ShapeDtypeStruct((8, 2, extra, 512), BF), jax.ShapeDtypeStruct((1024, 512), BF)]
        out_specs += [pl.BlockSpec((2, 2, extra, 512), lambda s, m: (m[s], 0, 0, 0)), whole((1024, 512))]
    else:
        operands.append(states)
        in_specs.append(whole((1024, 512)))
        out_shape += [jax.ShapeDtypeStruct((size, 512), BF) for size in CHUNKS]
        out_specs += [whole((size, 512)) for size in CHUNKS]
    return pl.pallas_call(
        lambda *refs: matmul_kernel(extra, *refs),
        out_shape=out_shape,
        grid_spec=pltpu.PrefetchScalarGridSpec(
            num_scalar_prefetch=1,
            grid=(4,),
            in_specs=in_specs,
            out_specs=out_specs,
            scratch_shapes=[pltpu.VMEM((1024, 512), F32)],
        ),
        compiler_params=BIG,
        cost_estimate=pl.CostEstimate(
            flops=4_300_000_000, bytes_accessed=18 << 20, transcendentals=0
        ),
        name="matmul",
    )(meta, *operands)


def project_kernel(meta, g0, g1, g3, fa, fb, own_ref, peer_ref, give_ref, keep_ref, far_ref):
    core = meta[1]
    half = fa.shape[0]
    dims = (((1,), (1,)), ((), ()))
    step = pl.program_id(0)

    @pl.when(step == 0)
    def _():
        far_ref[:half] = fa[...]
        far_ref[half:] = fb[...]

    def side(out_ref):
        for w_ref, at in ((own_ref, core), (peer_ref, 1 - core)):
            cols = pl.ds(pl.multiple_of(at * 256, 256), 256)
            acc = lax.dot_general(g0[...], w_ref[0, 0], dims, preferred_element_type=F32)
            acc += lax.dot_general(g1[...], w_ref[0, 1], dims, preferred_element_type=F32)
            acc += lax.dot_general(far_ref[...], w_ref[0, 2], dims, preferred_element_type=F32)
            acc += lax.dot_general(g3[...], w_ref[0, 3], dims, preferred_element_type=F32)
            out_ref[:, cols] = acc.astype(out_ref.dtype)

    @pl.when(step == 0)
    def _():
        side(give_ref)

    @pl.when(step == 1)
    def _():
        side(keep_ref)


def project(meta, gs, w_own, w_peer):
    size = gs[0].shape[0]
    wspec = pl.BlockSpec((1, 4, 256, 512), lambda s, m: (jnp.bitwise_xor(m[0], s), 0, 0, 0))
    return pl.pallas_call(
        project_kernel,
        out_shape=[
            jax.ShapeDtypeStruct((size, 512), BF),
            jax.ShapeDtypeStruct((size, 512), F32),
        ],
        grid_spec=pltpu.PrefetchScalarGridSpec(
            num_scalar_prefetch=1,
            grid=(2,),
            in_specs=[whole(g.shape) for g in gs] + [wspec, wspec],
            out_specs=[whole((size, 512))] * 2,
            scratch_shapes=[pltpu.VMEM((size, 512), BF)],
        ),
        compiler_params=BIG,
        cost_estimate=pl.CostEstimate(
            flops=size * 2048 * 2048, bytes_accessed=8 << 20, transcendentals=0
        ),
        name="project",
    )(meta, *gs, w_own, w_peer)


def gather_z_first(q):
    other = send_z(q)
    pair = jnp.stack([q, other])
    left = send_x(pair, 1)
    right = send_x(pair, -1)
    far_own = send_x(left[0], 1)
    far_other = send_x(right[1], -1)
    near = jnp.concatenate([pair, left, right])
    far = jnp.stack([far_own, far_other])
    return near, send_core(near), far, send_core(far)


def on_device(
    tokens, input_source, branch_source, output_source, gates_source, decay_param, block_order
):
    x, z, core, y, zh = position()
    own_blocks = lax.dynamic_slice_in_dim(block_order, (y * 2 + zh) * 2, 2)

    def section(w):
        picked = jnp.take(w.astype(BF), block_order, axis=1)
        return jnp.transpose(picked, (1, 0, 2)).reshape(8, 64, 256)

    gates_picked = jnp.take(gates_source.astype(BF), block_order, axis=1)
    gates_flat = jnp.transpose(gates_picked.reshape(2, 8, 2, 16, 32), (1, 0, 2, 3, 4)).reshape(8, 8, 256)
    packed = jnp.concatenate(
        [section(input_source), section(branch_source), section(output_source), gates_flat], axis=1
    )
    swapped = lax.all_to_all(packed, "tensor", 0, 0, tiled=True)

    def piece(n):
        part = swapped[:, n * 64 : (n + 1) * 64].reshape(8, 2, 32, 256)
        return jnp.transpose(part, (3, 1, 0, 2)).reshape(256, 512)

    gate_part = swapped[:, 192:200].reshape(8, 2, 2, 16, 32)
    gate_rows = jnp.transpose(gate_part, (1, 3, 2, 0, 4)).reshape(32, 512)

    pair_meta = slot_meta((0, -1, 1, 2))
    row_meta = slot_meta((0, 1, 2, 3))

    q = piece(2)
    left = send_x(q, 1)
    right = send_x(q, -1)
    far_top = send_x(left[:128], 1)
    far_low = send_x(right[128:], -1)
    row = jnp.stack([q, right, jnp.concatenate([far_top, far_low]), left])
    other_row = send_z(row)

    def along_y(row):
        got = [lax.dynamic_index_in_dim(row, (y - x) & 3, 0, keepdims=False)]
        for r in (1, 2, 3):
            block = lax.dynamic_index_in_dim(row, (y - r - x) & 3, 0, keepdims=False)
            got.append(send_y(block, -r))
        return jnp.stack(got)

    w_own = jnp.stack([along_y(row), along_y(other_row)])
    w_peer = send_core(w_own)
    out_peers = (send_core(row), send_core(other_row))

    in_parts = gather_z_first(jnp.concatenate([piece(0), gate_rows]))
    br_parts = gather_z_first(piece(1))

    w, g, branch_in = matmul(pair_meta, tokens, in_parts, 32)
    input_serve = w.reshape(4096, 512)
    rate = -8.0 * jax.nn.softplus(jnp.take(decay_param, own_blocks, axis=0)).reshape(1, 512)
    states, gates_serve = gate_scan(branch_in, g.reshape(16, 32, 512), rate)
    w, *gated = matmul(pair_meta, tokens, br_parts, 0, states)
    branch_serve = w.reshape(4096, 512)
    output_serve = place(row_meta, (row, other_row), out_peers)

    give_meta = jnp.stack([(1 - zh) ^ z, core]).astype(jnp.int32)
    parts = []
    for g in gated:
        half = g.shape[0] // 2
        below = send_y(g, 1)
        above = send_y(g, -1)
        far_a = send_y(below[:half], 1)
        far_b = send_y(above[half:], -1)
        terms = (g, above, below, far_a, far_b)
        give, keep = project(give_meta, terms, w_own, w_peer)
        got = send_zhi(give)
        parts.append((keep + got.astype(F32)).astype(BF))
    mixed = jnp.concatenate(parts)
    return (mixed, input_serve, branch_serve, output_serve, gates_serve)


def solution(mesh):
    return jax.shard_map(
        on_device,
        mesh=mesh,
        in_specs=(
            P("fsdp", None),
            P("tensor", None, "fsdp"),
            P("tensor", None, "fsdp"),
            P("tensor", None, "fsdp"),
            P(None, None, "fsdp", "tensor"),
            P(),
            P(),
        ),
        out_specs=(
            P("fsdp", "tensor"),
            P(None, "tensor"),
            P(None, "tensor"),
            P(None, "tensor"),
            P(None, "tensor", None, None),
        ),
        check_vma=False,
    )
```

```python
import jax
import jax.numpy as jnp
from jax import lax
from jax.experimental import pallas as pl
from jax.experimental.pallas import tpu as pltpu
from jax.sharding import PartitionSpec as P


BF = jnp.bfloat16
F32 = jnp.float32


def fsdp_perm(dx=0, dz=0, dc=0):
    out = []
    for f in range(16):
        x, z, c = f // 4, (f // 2) % 2, f % 2
        out.append((f, (((x + dx) % 4) * 2 + (z ^ dz)) * 2 + (c ^ dc)))
    return out


def tensor_perm(dy=0, dz=0):
    return [(t, ((t // 2 + dy) % 4) * 2 + ((t % 2) ^ dz)) for t in range(8)]


CH = 512
BIG = pltpu.CompilerParams(vmem_limit_bytes=60 << 20)


def scan_kernel(bi_ref, g_ref, rate_ref, out_ref, gates_ref):
    rate = rate_ref[...]
    low = lax.broadcasted_iota(jnp.int32, (CH // 8, 8, 256), 1) < 4
    w_r = g_ref[:, :16].reshape(256, 256)
    w_i = g_ref[:, 16:].reshape(256, 256)
    gates_ref[0, 0] = w_r.T
    gates_ref[1, 0] = w_i.T

    def chunk(n, carry):
        rows = pl.ds(pl.multiple_of(n * CH, CH), CH)
        bi = bi_ref[rows, :]
        pre_r = jnp.dot(bi, g_ref[:, :16].reshape(256, 256), preferred_element_type=F32)
        pre_i = jnp.dot(bi, g_ref[:, 16:].reshape(256, 256), preferred_element_type=F32)
        a = jnp.exp(rate * jax.nn.sigmoid(pre_r))
        d = jnp.sqrt(1.0 - a * a) * (jax.nn.sigmoid(pre_i) * bi.astype(F32))
        a = a.reshape(CH // 8, 8, 256)
        d = d.reshape(CH // 8, 8, 256)
        a_prev = jnp.where(low, 1.0, pltpu.roll(a, 4, 1))
        d_prev = jnp.where(low, 0.0, pltpu.roll(d, 4, 1))
        d = a * d_prev + d
        a = a * a_prev
        a_end = jnp.where(low, pltpu.roll(a, 4, 1), a)
        d_end = jnp.where(low, pltpu.roll(d, 4, 1), d)
        states = []
        for k in range(CH // 8):
            states.append(a[k] * carry + d[k])
            carry = a_end[k] * carry + d_end[k]
        out_ref[rows, :] = jnp.concatenate(states, axis=0)
        return carry

    lax.fori_loop(0, 1024 // CH, chunk, jnp.zeros((8, 256), F32))


def gate_scan(branch_in, gates, rate):
    return pl.pallas_call(
        scan_kernel,
        out_shape=[
            jax.ShapeDtypeStruct((1024, 512), F32),
            jax.ShapeDtypeStruct((2, 2, 256, 256), BF),
        ],
        grid=(2,),
        in_specs=[
            pl.BlockSpec((1024, 256), lambda j: (0, j)),
            pl.BlockSpec((16, 32, 256), lambda j: (0, 0, j)),
            pl.BlockSpec((1, 256), lambda j: (0, j)),
        ],
        out_specs=[
            pl.BlockSpec((1024, 256), lambda j: (0, j)),
            pl.BlockSpec((2, 1, 256, 256), lambda j: (0, j, 0, 0)),
        ],
        compiler_params=BIG,
        cost_estimate=pl.CostEstimate(
            flops=8_000_000_000, bytes_accessed=4 << 20, transcendentals=4 << 20
        ),
        name="gate_scan",
    )(branch_in, gates, rate)


def send_x(a, dx):
    return lax.ppermute(a, "fsdp", fsdp_perm(dx=dx))


def send_z(a):
    return lax.ppermute(a, "fsdp", fsdp_perm(dz=1))


def send_core(a):
    return lax.ppermute(a, "fsdp", fsdp_perm(dc=1))


def send_y(a, dy):
    return lax.ppermute(a, "tensor", tensor_perm(dy=dy))


def send_zhi(a):
    return lax.ppermute(a, "tensor", tensor_perm(dz=1))


CHUNKS = (384, 384, 256)


def position():
    f = lax.axis_index("fsdp")
    t = lax.axis_index("tensor")
    return f // 4, (f // 2) % 2, f % 2, t // 2, t % 2


def slot_meta(dx):
    x, z, core, _, _ = position()
    at = (x + jnp.array(dx, jnp.int32) + 4) & 3
    return jnp.concatenate([at, core[None], z[None]]).astype(jnp.int32)


def put(w_ref, core, z, owns, peers):
    for j in range(2):
        at = jnp.bitwise_xor(z, j)
        w_ref[at, core] = owns[j]
        w_ref[at, 1 - core] = peers[j]


def place_kernel(meta, own0, own1, peer0, peer1, w_ref):
    core, z = meta[4], meta[5]
    put(w_ref, core, z, (own0[0], own1[0]), (peer0[0], peer1[0]))


def place(meta, owns, peers):
    src = pl.BlockSpec((1, 256, 512), lambda s, m: (s, 0, 0))
    w = pl.pallas_call(
        place_kernel,
        out_shape=jax.ShapeDtypeStruct((8, 2, 256, 512), BF),
        grid_spec=pltpu.PrefetchScalarGridSpec(
            num_scalar_prefetch=1,
            grid=(4,),
            in_specs=[src] * 4,
            out_specs=pl.BlockSpec((2, 2, 256, 512), lambda s, m: (m[s], 0, 0, 0)),
        ),
        compiler_params=BIG,
        cost_estimate=pl.CostEstimate(flops=4_000_000, bytes_accessed=8 << 20, transcendentals=0),
        name="place",
    )(meta, *owns, *peers)
    return w.reshape(4096, 512)


def matmul_kernel(extra, meta, tok_ref, near_ref, near_peer_ref, far_ref, far_peer_ref, *refs):
    if extra:
        w_ref, g_ref, out_ref, acc_ref = refs
    else:
        state_ref, w_ref, *out_refs, acc_ref = refs
    core, z = meta[4], meta[5]
    step = pl.program_id(0)

    def put_all(own_ref, peer_ref):
        put(w_ref, core, z, (own_ref[0, :256], own_ref[1, :256]), (peer_ref[0, :256], peer_ref[1, :256]))
        if extra:
            put(g_ref, core, z, (own_ref[0, 256:], own_ref[1, 256:]), (peer_ref[0, 256:], peer_ref[1, 256:]))

    @pl.when(step < 3)
    def _():
        put_all(near_ref, near_peer_ref)

    @pl.when(step == 3)
    def _():
        put_all(far_ref, far_peer_ref)

    w = w_ref[...].reshape(1024, 512)

    @pl.when(step == 0)
    def _():
        acc_ref[...] = jnp.dot(tok_ref[...], w, preferred_element_type=F32)

    @pl.when(step > 0)
    def _():
        acc_ref[...] += jnp.dot(tok_ref[...], w, preferred_element_type=F32)

    @pl.when(step == 3)
    def _():
        if extra:
            out_ref[...] = acc_ref[...].astype(BF)
        else:
            base = 0
            for size, part_ref in zip(CHUNKS, out_refs):

                def rows_step(n, _, base=base, part_ref=part_ref):
                    rows = pl.ds(pl.multiple_of(base + n * 32, 32), 32)
                    value = state_ref[rows, :] * jax.nn.gelu(acc_ref[rows, :], approximate=True)
                    part_ref[pl.ds(pl.multiple_of(n * 32, 32), 32), :] = value.astype(BF)
                    return 0

                lax.fori_loop(0, size // 32, rows_step, 0)
                base += size


def whole(shape):
    return pl.BlockSpec(shape, lambda s, m: (0,) * len(shape))


def matmul(meta, tokens, parts, extra, states=None):
    rows = 256 + extra
    near = pl.BlockSpec((2, rows, 512), lambda s, m: (jnp.minimum(s, 2), 0, 0))
    operands = [tokens, *parts]
    in_specs = [pl.BlockSpec((1024, 1024), lambda s, m: (0, m[s])), near, near]
    in_specs += [whole((2, rows, 512))] * 2
    out_shape = [jax.ShapeDtypeStruct((8, 2, 256, 512), BF)]
    out_specs = [pl.BlockSpec((2, 2, 256, 512), lambda s, m: (m[s], 0, 0, 0))]
    if extra:
        out_shape += [jax.ShapeDtypeStruct((8, 2, extra, 512), BF), jax.ShapeDtypeStruct((1024, 512), BF)]
        out_specs += [pl.BlockSpec((2, 2, extra, 512), lambda s, m: (m[s], 0, 0, 0)), whole((1024, 512))]
    else:
        operands.append(states)
        in_specs.append(whole((1024, 512)))
        out_shape += [jax.ShapeDtypeStruct((size, 512), BF) for size in CHUNKS]
        out_specs += [whole((size, 512)) for size in CHUNKS]
    return pl.pallas_call(
        lambda *refs: matmul_kernel(extra, *refs),
        out_shape=out_shape,
        grid_spec=pltpu.PrefetchScalarGridSpec(
            num_scalar_prefetch=1,
            grid=(4,),
            in_specs=in_specs,
            out_specs=out_specs,
            scratch_shapes=[pltpu.VMEM((1024, 512), F32)],
        ),
        compiler_params=BIG,
        cost_estimate=pl.CostEstimate(
            flops=4_300_000_000, bytes_accessed=18 << 20, transcendentals=0
        ),
        name="matmul",
    )(meta, *operands)


def project_kernel(meta, g0, g1, g2, g3, own_ref, peer_ref, give_ref, keep_ref):
    core = meta[1]
    dims = (((1,), (1,)), ((), ()))
    step = pl.program_id(0)

    def side(out_ref):
        for w_ref, at in ((own_ref, core), (peer_ref, 1 - core)):
            cols = pl.ds(pl.multiple_of(at * 256, 256), 256)
            acc = lax.dot_general(g0[...], w_ref[0, 0], dims, preferred_element_type=F32)
            acc += lax.dot_general(g1[...], w_ref[0, 1], dims, preferred_element_type=F32)
            acc += lax.dot_general(g2[...], w_ref[0, 2], dims, preferred_element_type=F32)
            acc += lax.dot_general(g3[...], w_ref[0, 3], dims, preferred_element_type=F32)
            out_ref[:, cols] = acc.astype(out_ref.dtype)

    @pl.when(step == 0)
    def _():
        side(give_ref)

    @pl.when(step == 1)
    def _():
        side(keep_ref)


def project(meta, gs, w_own, w_peer):
    size = gs[0].shape[0]
    wspec = pl.BlockSpec((1, 4, 256, 512), lambda s, m: (jnp.bitwise_xor(m[0], s), 0, 0, 0))
    return pl.pallas_call(
        project_kernel,
        out_shape=[
            jax.ShapeDtypeStruct((size, 512), BF),
            jax.ShapeDtypeStruct((size, 512), F32),
        ],
        grid_spec=pltpu.PrefetchScalarGridSpec(
            num_scalar_prefetch=1,
            grid=(2,),
            in_specs=[whole(g.shape) for g in gs] + [wspec, wspec],
            out_specs=[whole((size, 512))] * 2,
        ),
        compiler_params=BIG,
        cost_estimate=pl.CostEstimate(
            flops=size * 2048 * 2048, bytes_accessed=8 << 20, transcendentals=0
        ),
        name="project",
    )(meta, *gs, w_own, w_peer)


def gather_z_first(name, q):
    other = send_z(q)
    pair = jnp.stack([q, other])
    left = send_x(pair, 1)
    right = send_x(pair, -1)
    if name == "in":
        far = jnp.stack([send_x(left[0], 1), send_x(right[1], -1)])
    else:
        far = send_x(pair, 2)
    near = jnp.concatenate([pair, left, right])
    return near, send_core(near), far, send_core(far)


def on_device(
    tokens, input_source, branch_source, output_source, gates_source, decay_param, block_order
):
    x, z, core, y, zh = position()
    own_blocks = lax.dynamic_slice_in_dim(block_order, (y * 2 + zh) * 2, 2)

    def section(w):
        picked = jnp.take(w.astype(BF), block_order, axis=1, mode="clip")
        return jnp.transpose(picked, (1, 0, 2)).reshape(8, 64, 256)

    gates_picked = jnp.take(gates_source.astype(BF), block_order, axis=1, mode="clip")
    gates_flat = jnp.transpose(gates_picked.reshape(2, 8, 2, 16, 32), (1, 0, 2, 3, 4)).reshape(8, 8, 256)
    packed = jnp.concatenate(
        [section(input_source), section(branch_source), section(output_source), gates_flat], axis=1
    )
    swapped = lax.all_to_all(packed, "tensor", 0, 0, tiled=True)

    def piece(n):
        part = swapped[:, n * 64 : (n + 1) * 64].reshape(8, 2, 32, 256)
        return jnp.transpose(part, (3, 1, 0, 2)).reshape(256, 512)

    gate_part = swapped[:, 192:200].reshape(8, 2, 2, 16, 32)
    gate_rows = jnp.transpose(gate_part, (1, 3, 2, 0, 4)).reshape(32, 512)

    pair_meta = slot_meta((0, -1, 1, 2))
    row_meta = slot_meta((0, 1, 2, 3))

    q = piece(2)
    left = send_x(q, 1)
    right = send_x(q, -1)
    far_top = send_x(left[:128], 1)
    far_low = send_x(right[128:], -1)
    row = jnp.stack([q, right, jnp.concatenate([far_top, far_low]), left])
    other_row = send_z(row)

    def along_y(row):
        got = [lax.dynamic_index_in_dim(row, (y - x) & 3, 0, keepdims=False)]
        for r in (1, 2, 3):
            block = lax.dynamic_index_in_dim(row, (y - r - x) & 3, 0, keepdims=False)
            got.append(send_y(block, -r))
        return jnp.stack(got)

    w_own = jnp.stack([along_y(row), along_y(other_row)])
    w_peer = send_core(w_own)
    out_peers = (send_core(row), send_core(other_row))

    in_parts = gather_z_first("in", jnp.concatenate([piece(0), gate_rows]))
    br_parts = gather_z_first("br", piece(1))

    w, g, branch_in = matmul(pair_meta, tokens, in_parts, 32)
    input_serve = w.reshape(4096, 512)
    rate = -8.0 * jax.nn.softplus(jnp.take(decay_param, own_blocks, axis=0, mode="clip")).reshape(1, 512)
    states, gates_serve = gate_scan(branch_in, g.reshape(16, 32, 512), rate)
    w, *gated = matmul(pair_meta, tokens, br_parts, 0, states)
    branch_serve = w.reshape(4096, 512)
    output_serve = place(row_meta, (row, other_row), out_peers)

    give_meta = jnp.stack([(1 - zh) ^ z, core]).astype(jnp.int32)
    parts = []
    for n, g in enumerate(gated):
        below = send_y(g, 1)
        above = send_y(g, -1)
        if n == 0:
            far = send_y(below, 1)
        elif n == 1:
            far = send_y(above, -1)
        else:
            far = send_y(g, 2)
        terms = (g, above, far, below)
        give, keep = project(give_meta, terms, w_own, w_peer)
        got = send_zhi(give)
        parts.append((keep + got.astype(F32)).astype(BF))
    mixed = jnp.concatenate(parts)
    return (mixed, input_serve, branch_serve, output_serve, gates_serve)


def solution(mesh):
    return jax.shard_map(
        on_device,
        mesh=mesh,
        in_specs=(
            P("fsdp", None),
            P("tensor", None, "fsdp"),
            P("tensor", None, "fsdp"),
            P("tensor", None, "fsdp"),
            P(None, None, "fsdp", "tensor"),
            P(),
            P(),
        ),
        out_specs=(
            P("fsdp", "tensor"),
            P(None, "tensor"),
            P(None, "tensor"),
            P(None, "tensor"),
            P(None, "tensor", None, None),
        ),
        check_vma=False,
    )
```

```python
import jax
import jax.numpy as jnp
from jax import lax
from jax.experimental import pallas as pl
from jax.experimental.pallas import tpu as pltpu
from jax.sharding import PartitionSpec as P


BF = jnp.bfloat16
F32 = jnp.float32


def fsdp_perm(dx=0, dz=0, dc=0):
    out = []
    for f in range(16):
        x, z, c = f // 4, (f // 2) % 2, f % 2
        out.append((f, (((x + dx) % 4) * 2 + (z ^ dz)) * 2 + (c ^ dc)))
    return out


def tensor_perm(dy=0, dz=0):
    return [(t, ((t // 2 + dy) % 4) * 2 + ((t % 2) ^ dz)) for t in range(8)]


CH = 512
BIG = pltpu.CompilerParams(vmem_limit_bytes=28 << 20)


def scan_kernel(bi_ref, g_ref, rate_ref, out_ref, gates_ref):
    rate = rate_ref[...]
    low = lax.broadcasted_iota(jnp.int32, (CH // 8, 8, 256), 1) < 4
    w_r = g_ref[:, :16].reshape(256, 256)
    w_i = g_ref[:, 16:].reshape(256, 256)
    gates_ref[0, 0] = w_r.T
    gates_ref[1, 0] = w_i.T

    def chunk(n, carry):
        rows = pl.ds(pl.multiple_of(n * CH, CH), CH)
        bi = bi_ref[rows, :]
        pre_r = jnp.dot(bi, g_ref[:, :16].reshape(256, 256), preferred_element_type=F32)
        pre_i = jnp.dot(bi, g_ref[:, 16:].reshape(256, 256), preferred_element_type=F32)
        a = jnp.exp(rate * jax.nn.sigmoid(pre_r))
        d = jnp.sqrt(1.0 - a * a) * (jax.nn.sigmoid(pre_i) * bi.astype(F32))
        a = a.reshape(CH // 8, 8, 256)
        d = d.reshape(CH // 8, 8, 256)
        a_prev = jnp.where(low, 1.0, pltpu.roll(a, 4, 1))
        d_prev = jnp.where(low, 0.0, pltpu.roll(d, 4, 1))
        d = a * d_prev + d
        a = a * a_prev
        a_end = jnp.where(low, pltpu.roll(a, 4, 1), a)
        d_end = jnp.where(low, pltpu.roll(d, 4, 1), d)
        states = []
        for k in range(CH // 8):
            states.append(a[k] * carry + d[k])
            carry = a_end[k] * carry + d_end[k]
        out_ref[rows, :] = jnp.concatenate(states, axis=0)
        return carry

    lax.fori_loop(0, 1024 // CH, chunk, jnp.zeros((8, 256), F32))


def gate_scan(branch_in, gates, rate):
    return pl.pallas_call(
        scan_kernel,
        out_shape=[
            jax.ShapeDtypeStruct((1024, 512), F32),
            jax.ShapeDtypeStruct((2, 2, 256, 256), BF),
        ],
        grid=(2,),
        in_specs=[
            pl.BlockSpec((1024, 256), lambda j: (0, j)),
            pl.BlockSpec((16, 32, 256), lambda j: (0, 0, j)),
            pl.BlockSpec((1, 256), lambda j: (0, j)),
        ],
        out_specs=[
            pl.BlockSpec((1024, 256), lambda j: (0, j)),
            pl.BlockSpec((2, 1, 256, 256), lambda j: (0, j, 0, 0)),
        ],
        compiler_params=BIG,
        cost_estimate=pl.CostEstimate(
            flops=8_000_000_000, bytes_accessed=4 << 20, transcendentals=4 << 20
        ),
        name="gate_scan",
    )(branch_in, gates, rate)


def send_x(a, dx):
    return lax.ppermute(a, "fsdp", fsdp_perm(dx=dx))


def send_z(a):
    return lax.ppermute(a, "fsdp", fsdp_perm(dz=1))


def send_core(a):
    return lax.ppermute(a, "fsdp", fsdp_perm(dc=1))


def send_y(a, dy):
    return lax.ppermute(a, "tensor", tensor_perm(dy=dy))


def send_zhi(a):
    return lax.ppermute(a, "tensor", tensor_perm(dz=1))


CHUNKS = (384, 384, 256)


def position():
    f = lax.axis_index("fsdp")
    t = lax.axis_index("tensor")
    return f // 4, (f // 2) % 2, f % 2, t // 2, t % 2


def slot_meta(dx):
    x, z, core, _, _ = position()
    at = (x + jnp.array(dx, jnp.int32) + 4) & 3
    return jnp.concatenate([at, core[None], z[None]]).astype(jnp.int32)


def put(w_ref, core, z, owns, peers):
    for j in range(2):
        at = jnp.bitwise_xor(z, j)
        w_ref[at, core] = owns[j]
        w_ref[at, 1 - core] = peers[j]


def place_kernel(meta, own0, own1, peer0, peer1, w_ref):
    core, z = meta[4], meta[5]
    put(w_ref, core, z, (own0[0], own1[0]), (peer0[0], peer1[0]))


def place(meta, owns, peers):
    src = pl.BlockSpec((1, 256, 512), lambda s, m: (s, 0, 0))
    w = pl.pallas_call(
        place_kernel,
        out_shape=jax.ShapeDtypeStruct((8, 2, 256, 512), BF),
        grid_spec=pltpu.PrefetchScalarGridSpec(
            num_scalar_prefetch=1,
            grid=(4,),
            in_specs=[src] * 4,
            out_specs=pl.BlockSpec((2, 2, 256, 512), lambda s, m: (m[s], 0, 0, 0)),
        ),
        compiler_params=BIG,
        cost_estimate=pl.CostEstimate(flops=4_000_000, bytes_accessed=8 << 20, transcendentals=0),
        name="place",
    )(meta, *owns, *peers)
    return w.reshape(4096, 512)


def matmul_kernel(extra, meta, tok_ref, near_ref, near_peer_ref, far_ref, far_peer_ref, *refs):
    if extra:
        w_ref, g_ref, out_ref, acc_ref = refs
    else:
        state_ref, w_ref, *out_refs, acc_ref = refs
    core, z = meta[4], meta[5]
    step = pl.program_id(0)

    def put_all(own_ref, peer_ref):
        put(w_ref, core, z, (own_ref[0, :256], own_ref[1, :256]), (peer_ref[0, :256], peer_ref[1, :256]))
        if extra:
            put(g_ref, core, z, (own_ref[0, 256:], own_ref[1, 256:]), (peer_ref[0, 256:], peer_ref[1, 256:]))

    @pl.when(step < 3)
    def _():
        put_all(near_ref, near_peer_ref)

    @pl.when(step == 3)
    def _():
        put_all(far_ref, far_peer_ref)

    w = w_ref[...].reshape(1024, 512)
    if extra:
        tok = tok_ref[...]
    else:
        tok = tok_ref[:, pl.ds(pl.multiple_of(meta[step] * 1024, 1024), 1024)]

    @pl.when(step == 0)
    def _():
        acc_ref[...] = jnp.dot(tok, w, preferred_element_type=F32)

    @pl.when(step > 0)
    def _():
        acc_ref[...] += jnp.dot(tok, w, preferred_element_type=F32)

    @pl.when(step == 3)
    def _():
        if extra:
            out_ref[...] = acc_ref[...].astype(BF)
        else:
            base = 0
            for size, part_ref in zip(CHUNKS, out_refs):

                def rows_step(n, _, base=base, part_ref=part_ref):
                    rows = pl.ds(pl.multiple_of(base + n * 32, 32), 32)
                    value = state_ref[rows, :] * jax.nn.gelu(acc_ref[rows, :], approximate=True)
                    part_ref[pl.ds(pl.multiple_of(n * 32, 32), 32), :] = value.astype(BF)
                    return 0

                lax.fori_loop(0, size // 32, rows_step, 0)
                base += size


def whole(shape):
    return pl.BlockSpec(shape, lambda s, m: (0,) * len(shape))


def matmul(meta, tokens, parts, extra, states=None):
    rows = 256 + extra
    near = pl.BlockSpec((2, rows, 512), lambda s, m: (jnp.minimum(s, 2), 0, 0))
    operands = [tokens, *parts]
    blocked = pl.BlockSpec((1024, 1024), lambda s, m: (0, m[s]))
    in_specs = [blocked if extra else pl.BlockSpec(memory_space=pltpu.VMEM), near, near]
    in_specs += [whole((2, rows, 512))] * 2
    out_shape = [jax.ShapeDtypeStruct((8, 2, 256, 512), BF)]
    out_specs = [pl.BlockSpec((2, 2, 256, 512), lambda s, m: (m[s], 0, 0, 0))]
    if extra:
        out_shape += [jax.ShapeDtypeStruct((8, 2, extra, 512), BF), jax.ShapeDtypeStruct((1024, 512), BF)]
        out_specs += [pl.BlockSpec((2, 2, extra, 512), lambda s, m: (m[s], 0, 0, 0)), whole((1024, 512))]
    else:
        operands.append(states)
        in_specs.append(whole((1024, 512)))
        out_shape += [jax.ShapeDtypeStruct((size, 512), BF) for size in CHUNKS]
        out_specs += [whole((size, 512)) for size in CHUNKS]
    return pl.pallas_call(
        lambda *refs: matmul_kernel(extra, *refs),
        out_shape=out_shape,
        grid_spec=pltpu.PrefetchScalarGridSpec(
            num_scalar_prefetch=1,
            grid=(4,),
            in_specs=in_specs,
            out_specs=out_specs,
            scratch_shapes=[pltpu.VMEM((1024, 512), F32)],
        ),
        compiler_params=pltpu.CompilerParams(vmem_limit_bytes=(58 if extra else 28) << 20),
        cost_estimate=pl.CostEstimate(
            flops=4_300_000_000, bytes_accessed=18 << 20, transcendentals=0
        ),
        name="matmul",
    )(meta, *operands)


def project_kernel(meta, g0, g1, g2, g3, own_ref, peer_ref, give_ref, keep_ref):
    core = meta[1]
    dims = (((1,), (1,)), ((), ()))
    step = pl.program_id(0)

    def side(out_ref):
        for w_ref, at in ((own_ref, core), (peer_ref, 1 - core)):
            cols = pl.ds(pl.multiple_of(at * 256, 256), 256)
            acc = lax.dot_general(g0[...], w_ref[0, 0], dims, preferred_element_type=F32)
            acc += lax.dot_general(g1[...], w_ref[0, 1], dims, preferred_element_type=F32)
            acc += lax.dot_general(g2[...], w_ref[0, 2], dims, preferred_element_type=F32)
            acc += lax.dot_general(g3[...], w_ref[0, 3], dims, preferred_element_type=F32)
            out_ref[:, cols] = acc.astype(out_ref.dtype)

    @pl.when(step == 0)
    def _():
        side(give_ref)

    @pl.when(step == 1)
    def _():
        side(keep_ref)


def project(meta, gs, w_own, w_peer, limit):
    size = gs[0].shape[0]
    wspec = pl.BlockSpec((1, 4, 256, 512), lambda s, m: (jnp.bitwise_xor(m[0], s), 0, 0, 0))
    return pl.pallas_call(
        project_kernel,
        out_shape=[
            jax.ShapeDtypeStruct((size, 512), BF),
            jax.ShapeDtypeStruct((size, 512), F32),
        ],
        grid_spec=pltpu.PrefetchScalarGridSpec(
            num_scalar_prefetch=1,
            grid=(2,),
            in_specs=[whole(g.shape) for g in gs] + [wspec, wspec],
            out_specs=[whole((size, 512))] * 2,
        ),
        compiler_params=pltpu.CompilerParams(vmem_limit_bytes=limit << 20),
        cost_estimate=pl.CostEstimate(
            flops=size * 2048 * 2048, bytes_accessed=8 << 20, transcendentals=0
        ),
        name="project",
    )(meta, *gs, w_own, w_peer)


def pack_kernel(meta, in_ref, br_ref, out_ref, g_ref, *refs):
    sends, turned = refs[:8], refs[8]
    for n, w_ref in enumerate((in_ref, br_ref, out_ref)):
        turned[n] = jnp.swapaxes(w_ref[...], 0, 1).astype(BF)
    for r in range(8):
        peer = jnp.bitwise_xor(meta[16], r)
        blocks = [meta[2 * peer + j] for j in range(2)]
        for n in range(3):
            for j in range(2):
                sends[r][n * 64 + j * 32 : n * 64 + j * 32 + 32, :] = turned[n, blocks[j]]
        parts = [g_ref[g, blocks[j]] for g in range(2) for j in range(2)]
        gates = jnp.concatenate(parts, axis=1)
        sends[r][192:208, :] = jnp.concatenate([gates, gates], axis=1).astype(BF)


def pack(meta, sources, gates):
    return pl.pallas_call(
        pack_kernel,
        out_shape=[jax.ShapeDtypeStruct((208, 256), BF)] * 8,
        grid_spec=pltpu.PrefetchScalarGridSpec(
            num_scalar_prefetch=1,
            grid=(1,),
            in_specs=[whole((32, 16, 256))] * 3 + [whole((2, 16, 16, 32))],
            out_specs=[whole((208, 256))] * 8,
            scratch_shapes=[pltpu.VMEM((3, 16, 32, 256), BF)],
        ),
        cost_estimate=pl.CostEstimate(flops=4_000_000, bytes_accessed=3 << 20, transcendentals=0),
        name="pack",
    )(meta, *sources, gates)


def unpack_kernel(meta, *refs):
    got, (in_ref, br_ref, out_ref), rows, gates = refs[:8], refs[8:11], refs[11], refs[12]
    for r in range(8):
        peer = jnp.bitwise_xor(meta[16], r)
        for n in range(3):
            for j in range(2):
                rows[n, j, peer] = got[r][n * 64 + j * 32 : n * 64 + j * 32 + 32, :]
        gates[peer] = got[r][192:208, :128].astype(F32)
    for n, ref in enumerate((in_ref, br_ref, out_ref)):
        for j in range(2):
            ref[:256, j * 256 : j * 256 + 256] = rows[n, j].reshape(256, 256).T
    for g in range(2):
        for j in range(2):
            at = (g * 2 + j) * 32
            line = jnp.concatenate([gates[p][:, at : at + 32] for p in range(8)], axis=1)
            in_ref[256 + g * 16 : 272 + g * 16, j * 256 : j * 256 + 256] = line.astype(BF)


def unpack(meta, got):
    return pl.pallas_call(
        unpack_kernel,
        out_shape=[jax.ShapeDtypeStruct((rows, 512), BF) for rows in (288, 256, 256)],
        grid_spec=pltpu.PrefetchScalarGridSpec(
            num_scalar_prefetch=1,
            grid=(1,),
            in_specs=[whole((208, 256))] * 8,
            out_specs=[whole((rows, 512)) for rows in (288, 256, 256)],
            scratch_shapes=[pltpu.VMEM((3, 2, 8, 32, 256), BF), pltpu.VMEM((8, 16, 128), F32)],
        ),
        cost_estimate=pl.CostEstimate(flops=4_000_000, bytes_accessed=3 << 20, transcendentals=0),
        name="unpack",
    )(meta, *got)


def gather_z_first(name, q):
    other = send_z(q)
    pair = jnp.stack([q, other])
    left = send_x(pair, 1)
    right = send_x(pair, -1)
    if name == "in":
        far = jnp.stack([send_x(left[0], 1), send_x(right[1], -1)])
    else:
        far = send_x(pair, 2)
    near = jnp.concatenate([pair, left, right])
    return near, send_core(near), far, send_core(far)


def on_device(
    tokens, input_source, branch_source, output_source, gates_source, decay_param, block_order
):
    x, z, core, y, zh = position()
    own_blocks = lax.dynamic_slice_in_dim(block_order, (y * 2 + zh) * 2, 2)

    pack_meta = jnp.concatenate([block_order, lax.axis_index("tensor")[None]]).astype(jnp.int32)
    sends = pack(pack_meta, (input_source, branch_source, output_source), gates_source)
    got = [sends[0]]
    for r in range(1, 8):
        got.append(lax.ppermute(sends[r], "tensor", [(t, t ^ r) for t in range(8)]))
    in_piece, br_piece, out_piece = unpack(pack_meta, got)

    pair_meta = slot_meta((0, -1, 1, 2))
    row_meta = slot_meta((0, 1, 2, 3))

    q = out_piece
    left = send_x(q, 1)
    right = send_x(q, -1)
    far_top = send_x(left[:128], 1)
    far_low = send_x(right[128:], -1)
    row = jnp.stack([q, right, jnp.concatenate([far_top, far_low]), left])
    other_row = send_z(row)

    def along_y(row):
        got = [lax.dynamic_index_in_dim(row, (y - x) & 3, 0, keepdims=False)]
        for r in (1, 2, 3):
            block = lax.dynamic_index_in_dim(row, (y - r - x) & 3, 0, keepdims=False)
            got.append(send_y(block, -r))
        return jnp.stack(got)

    w_own = jnp.stack([along_y(row), along_y(other_row)])
    w_peer = send_core(w_own)
    out_peers = (send_core(row), send_core(other_row))

    in_parts = gather_z_first("in", in_piece)
    br_parts = gather_z_first("br", br_piece)

    w, g, branch_in = matmul(pair_meta, tokens, in_parts, 32)
    input_serve = w.reshape(4096, 512)
    rate = -8.0 * jax.nn.softplus(jnp.take(decay_param, own_blocks, axis=0, mode="clip")).reshape(1, 512)
    states, gates_serve = gate_scan(branch_in, g.reshape(16, 32, 512), rate)
    held = pltpu.with_memory_space_constraint(tokens, pltpu.VMEM)
    w, *gated = matmul(pair_meta, held, br_parts, 0, states)
    branch_serve = w.reshape(4096, 512)
    output_serve = place(row_meta, (row, other_row), out_peers)

    give_meta = jnp.stack([(1 - zh) ^ z, core]).astype(jnp.int32)
    parts = []
    for n, g in enumerate(gated):
        below = send_y(g, 1)
        above = send_y(g, -1)
        if n == 0:
            far = send_y(below, 1)
        elif n == 1:
            far = send_y(above, -1)
        else:
            far = send_y(g, 2)
        terms = (g, above, far, below)
        give, keep = project(give_meta, terms, w_own, w_peer, (28, 58, 28)[n])
        got = send_zhi(give)
        parts.append((keep + got.astype(F32)).astype(BF))
    mixed = jnp.concatenate(parts)
    return (mixed, input_serve, branch_serve, output_serve, gates_serve)


def solution(mesh):
    return jax.shard_map(
        on_device,
        mesh=mesh,
        in_specs=(
            P("fsdp", None),
            P("tensor", None, "fsdp"),
            P("tensor", None, "fsdp"),
            P("tensor", None, "fsdp"),
            P(None, None, "fsdp", "tensor"),
            P(),
            P(),
        ),
        out_specs=(
            P("fsdp", "tensor"),
            P(None, "tensor"),
            P(None, "tensor"),
            P(None, "tensor"),
            P(None, "tensor", None, None),
        ),
        check_vma=False,
    )
```
